32 devices in a mesh: seq: 8 (over z, y), grp: 4 (over x, core).
Axes of the slice: x: 2, y: 2, z: 4, core: 2. Of those that a mesh axis runs over, the one named last changes fastest.
Arguments:
- tokens: bfloat16 [4096, 2560], P('seq'), may hold values from -6 to 6
- norm_gain: float32 [2560], replicated, may hold values from 0.25 to 1.75
- inner_weight: bfloat16 [2560, 2, 5120], P(None, None, ('grp', 'seq')), may hold values from -0.125 to 0.125
- state_weight: bfloat16 [2560, 2, 128], replicated, may hold values from -0.125 to 0.125
- step_weight: bfloat16 [2560, 80], P(None, 'grp'), may hold values from -0.125 to 0.125
- step_bias: float32 [80], P('grp'), may hold values from -1 to 1
- decay_rate: float32 [80], P('grp'), may hold values from 4.8828124e-06 to 0.05
- skip_scale: float32 [80], P('grp'), may hold values from 0.5 to 1.5
- conv_inner: bfloat16 [4, 5120], P(None, 'grp'), may hold values from -3 to 3
- conv_state: bfloat16 [4, 2, 128], replicated, may hold values from -3 to 3
- out_gain: float32 [5120], P('grp'), may hold values from 0.25 to 1.75
- out_weight: bfloat16 [5120, 2560], P(None, 'grp'), may hold values from -0.078125 to 0.078125
Outputs:
- mixed: bfloat16 [4096, 2560], P('seq', 'grp')
The draws below stay inside these ranges and needn't reach their ends.
All inputs are finite; a program needn't handle non-finite values.
Results may differ from the reference program's by a relative error of at most 0.0075.
Values may be sent and summed in bfloat16 or wider, within the bound.
No kernel may reach another device: no remote copies, remote signals or barrier semaphores. Data moves between devices by JAX's collectives and lax.ppermute only.
A program may use at most 64 MiB of HBM per device.

```python
import math
from functools import partial
import jax
import jax.numpy as jnp
from jax import lax

D = 2560
D_INNER = 5120
HEADS = 80
HEAD_DIM = 64
D_STATE = 128
SPAN = 256
KERNEL = 4
SEQ_LEN = 4096


def block_levels(key, dims, cuts, smallest, high):
    def one(position, parts):
        draws = jax.random.uniform(jax.random.fold_in(jax.random.fold_in(key, 6), position), (parts,), jnp.float32, smallest / len(cuts), high / len(cuts))
        return jnp.repeat(jnp.exp(draws), dims[position] // parts).reshape((-1,) + (1,) * (len(dims) - position - 1))

    gain = one(*cuts[0])
    for cut in cuts[1:]:
        gain = gain * one(*cut)
    return gain


def bell_draw(rng, extent, scale, limit, split=(), held_as=jnp.bfloat16):
    level = block_levels(rng, extent, split, -0.22, 0.18) if split else 1.0
    drawn = jax.random.normal(rng, extent, jnp.float32) * scale * level
    return jnp.minimum(jnp.maximum(drawn, -limit), limit).astype(held_as)


def setup_inputs(seed: int = 0) -> dict:
    seeds = jax.random.split(jax.random.key(seed), 13)
    return {
        "tokens": bell_draw(seeds[0], (SEQ_LEN, D), 1.0, 6.0, ((0, 8),)),
        "norm_gain": jnp.clip(1.0 + 0.15 * jax.random.normal(seeds[1], (D,), jnp.float32), 0.25, 1.75),
        "inner_weight": bell_draw(seeds[2], (D, 2, D_INNER), D ** -0.5, 0.125, ((2, 32),)),
        "state_weight": bell_draw(seeds[3], (D, 2, D_STATE), D ** -0.5, 0.125),
        "step_weight": bell_draw(seeds[4], (D, HEADS), D ** -0.5, 0.125, ((1, 4),)),
        "step_bias": jnp.clip(jax.random.uniform(seeds[5], (HEADS,), jnp.float32, -1.0, 1.0) * block_levels(seeds[5], (HEADS,), ((0, 4),), -0.4, 0.0), -1.0, 1.0),
        "decay_rate": jnp.clip(jnp.exp(math.log(0.05) - 9.2340569 * jax.random.uniform(seeds[6], (HEADS,), jnp.float32) ** block_levels(seeds[6], (HEADS,), ((0, 4),), -0.2, 0.2)), 4.882812390860636e-06, 0.05),
        "skip_scale": jnp.clip(0.5 + 1.0 * jax.random.uniform(seeds[7], (HEADS,), jnp.float32) ** block_levels(seeds[7], (HEADS,), ((0, 4),), -0.2, 0.2), 0.5, 1.5),
        "conv_inner": bell_draw(seeds[8], (KERNEL, D_INNER), KERNEL ** -0.5, 3.0, ((1, 4),)),
        "conv_state": bell_draw(seeds[9], (KERNEL, 2, D_STATE), KERNEL ** -0.5, 3.0),
        "out_gain": jnp.clip(1.0 + 0.15 * jax.random.normal(seeds[10], (D_INNER,), jnp.float32), 0.25, 1.75),
        "out_weight": bell_draw(seeds[11], (D_INNER, D), D_INNER ** -0.5, 0.078125, ((1, 4),)),
    }


EPS = 1e-05
HIGH = lax.Precision.HIGHEST

def causal_conv(current, weight):
    width = weight.shape[0]
    before = jnp.zeros((width - 1,) + current.shape[1:], current.dtype)
    padded = jnp.concatenate([before, current], axis=0).astype(jnp.float32)
    length = current.shape[0]
    total = jnp.zeros(current.shape, jnp.float32)
    for offset in range(width):
        total = total + weight[offset].astype(jnp.float32) * padded[offset:offset + length]
    return jax.nn.silu(total).astype(jnp.bfloat16)

def span_step(rate, skip, state, inputs):
    xvals, bmat, cmat, delta = inputs
    logdec = -delta * rate[None, :]
    cumul = jnp.cumsum(logdec, axis=0)
    length = cumul.shape[0]
    scores = jnp.einsum('tn,sn->ts', cmat.astype(jnp.float32), bmat.astype(jnp.float32), precision=HIGH)
    lower = jnp.arange(length)[:, None] >= jnp.arange(length)[None, :]
    diffs = cumul.T[:, :, None] - cumul.T[:, None, :]
    decay = jnp.exp(jnp.where(lower[None], diffs, -jnp.inf))
    mixer = (scores[None] * decay * delta.T[:, None, :]).astype(jnp.bfloat16)
    xwide = xvals.astype(jnp.float32)
    intra = jnp.einsum('hts,shp->thp', mixer.astype(jnp.float32), xwide, precision=HIGH)
    inter = jnp.exp(cumul)[:, :, None] * jnp.einsum('tn,hpn->thp', cmat.astype(jnp.float32), state, precision=HIGH)
    output = intra + inter + skip[None, :, None] * xwide
    tail = jnp.exp(cumul[-1][None, :] - cumul) * delta
    weighted = (tail[:, :, None] * bmat.astype(jnp.float32)[:, None, :]).astype(jnp.bfloat16)
    update = jnp.einsum('shp,shn->hpn', xwide, weighted.astype(jnp.float32), precision=HIGH)
    new_state = jnp.exp(cumul[-1])[:, None, None] * state + update
    return (new_state, output)

def reference(tokens, norm_gain, inner_weight, state_weight, step_weight, step_bias, decay_rate, skip_scale, conv_inner, conv_state, out_gain, out_weight):
    length = tokens.shape[0]
    wide = tokens.astype(jnp.float32)
    normed = (wide * lax.rsqrt(lax.optimization_barrier(jnp.mean(wide * wide, axis=1, keepdims=True)) + EPS) * norm_gain).astype(jnp.bfloat16)
    normed_wide = normed.astype(jnp.float32)
    inner = jnp.dot(normed_wide, inner_weight.reshape(D, 2 * D_INNER).astype(jnp.float32), precision=HIGH)
    inner = inner.astype(jnp.bfloat16).reshape(length, 2, D_INNER)
    state_pre = jnp.dot(normed_wide, state_weight.reshape(D, 2 * D_STATE).astype(jnp.float32), precision=HIGH)
    state_pre = state_pre.astype(jnp.bfloat16).reshape(length, 2, D_STATE)
    delta = jax.nn.softplus(jnp.dot(normed_wide, step_weight.astype(jnp.float32), precision=HIGH) + step_bias)
    values = causal_conv(inner[:, 0, :], conv_inner)
    conv_out = causal_conv(state_pre, conv_state)
    blocks = length // SPAN
    xs_blocks = values.reshape(blocks, SPAN, HEADS, HEAD_DIM)
    b_blocks = conv_out[:, 0, :].reshape(blocks, SPAN, D_STATE)
    c_blocks = conv_out[:, 1, :].reshape(blocks, SPAN, D_STATE)
    d_blocks = delta.reshape(blocks, SPAN, HEADS)
    initial = jnp.zeros((HEADS, HEAD_DIM, D_STATE), jnp.float32)
    _, outputs = lax.scan(partial(span_step, decay_rate, skip_scale), initial, (xs_blocks, b_blocks, c_blocks, d_blocks))
    mixed_heads = outputs.reshape(length, D_INNER)
    gated = mixed_heads * jax.nn.silu(inner[:, 1, :].astype(jnp.float32))
    meansq = lax.optimization_barrier(jnp.mean(gated * gated, axis=1))
    scaled = (gated * out_gain).astype(jnp.bfloat16)
    projected = jnp.dot(scaled.astype(jnp.float32), out_weight.astype(jnp.float32), precision=HIGH)
    return (projected * lax.rsqrt(meansq + EPS)[:, None]).astype(jnp.bfloat16)
```

```python
from functools import partial

import jax
import jax.numpy as jnp
from jax import lax
from jax.experimental import pallas as pl
from jax.experimental.pallas import tpu as pltpu
from jax.sharding import PartitionSpec as P

SPAN = 256


EPS = 1e-05
HIGH = lax.Precision.HIGHEST


def from_behind(value, axis, steps):
    count = lax.axis_size(axis)
    leading, last = (max(0, -steps), min(count, count - steps))
    return lax.ppermute(value, axis, [(source, source + steps) for source in range(leading, last)])


def prefix(value, axis, combine, identity):
    length, place = (lax.axis_size(axis), lax.axis_index(axis))
    everything = jax.tree.map(lambda part: lax.all_gather(part, axis), value)
    start = jax.tree.map(
        lambda part, zero: jnp.broadcast_to(jnp.asarray(zero, part.dtype), part.shape),
        value,
        identity,
    )

    def step(k, before):
        reached = k < place
        new = combine(before, jax.tree.map(lambda part: part[k], everything))
        return jax.tree.map(lambda a, b: jnp.where(reached, a, b), new, before)

    return lax.fori_loop(0, length, step, start)


def conv_rows(before, current, weight):
    width = weight.shape[0]
    padded = jnp.concatenate([before, current], axis=0).astype(jnp.float32)
    length = current.shape[0]
    total = jnp.zeros(current.shape, jnp.float32)
    for offset in range(width):
        total = total + weight[offset].astype(jnp.float32) * padded[offset : offset + length]
    return jax.nn.silu(total).astype(jnp.bfloat16)


def span_step(rate, skip, state, inputs):
    xvals, bmat, cmat, delta = inputs
    logdec = -delta * rate[None, :]
    cumul = jnp.cumsum(logdec, axis=0)
    length = cumul.shape[0]
    scores = jnp.einsum("tn,sn->ts", cmat, bmat, preferred_element_type=jnp.float32)
    lower = jnp.arange(length)[:, None] >= jnp.arange(length)[None, :]
    diffs = cumul.T[:, :, None] - cumul.T[:, None, :]
    decay = jnp.exp(jnp.where(lower[None], diffs, -jnp.inf))
    mixer = (scores[None] * decay * delta.T[:, None, :]).astype(jnp.bfloat16)
    intra = jnp.einsum("hts,shp->thp", mixer, xvals, preferred_element_type=jnp.float32)
    inter = jnp.exp(cumul)[:, :, None] * jnp.einsum(
        "tn,hpn->thp", cmat.astype(jnp.float32), state, precision=HIGH
    )
    output = intra + inter + skip[None, :, None] * xvals.astype(jnp.float32)
    tail = jnp.exp(cumul[-1][None, :] - cumul) * delta
    weighted = (tail[:, :, None] * bmat.astype(jnp.float32)[:, None, :]).astype(jnp.bfloat16)
    update = jnp.einsum("shp,shn->hpn", xvals, weighted, preferred_element_type=jnp.float32)
    new_state = jnp.exp(cumul[-1])[:, None, None] * state + update
    return (new_state, output)


def plain_body(
    tokens,
    norm_gain,
    inner_weight,
    state_weight,
    step_weight,
    step_bias,
    decay_rate,
    skip_scale,
    conv_inner,
    conv_state,
    out_gain,
    out_weight,
):
    tok_rows = tokens.shape[0]
    model_width = tokens.shape[1]
    wide = tokens.astype(jnp.float32)
    normed = (
        wide * lax.rsqrt(jnp.mean(wide * wide, axis=1, keepdims=True) + EPS) * norm_gain
    ).astype(jnp.bfloat16)
    piece = lax.all_gather(inner_weight, "seq", axis=2, tiled=True)
    count = piece.shape[2]
    flat = piece.reshape(piece.shape[0], 2 * count)
    result = jnp.dot(normed, flat, preferred_element_type=jnp.float32).astype(jnp.bfloat16)
    inner = result.reshape(tok_rows, 2, count)
    state_flat = state_weight.reshape(model_width, -1)
    state_pre = (
        jnp.dot(normed, state_flat, preferred_element_type=jnp.float32)
        .astype(jnp.bfloat16)
        .reshape(tok_rows, 2, -1)
    )
    delta = jax.nn.softplus(
        jnp.dot(normed, step_weight, preferred_element_type=jnp.float32) + step_bias
    )
    inner_values = inner[:, 0, :]
    width = conv_inner.shape[0]
    first_kept = tok_rows - width + 1
    before_values, before_state = from_behind(
        (inner_values[first_kept:], state_pre[first_kept:]), "seq", 1
    )
    values = conv_rows(before_values, inner_values, conv_inner)
    conv_out = conv_rows(before_state, state_pre, conv_state)
    heads_here = delta.shape[1]
    head_width = values.shape[1] // heads_here
    state_width = conv_out.shape[2]
    blocks = tok_rows // SPAN
    xs_blocks = values.reshape(blocks, SPAN, heads_here, head_width)
    b_blocks = conv_out[:, 0, :].reshape(blocks, SPAN, state_width)
    c_blocks = conv_out[:, 1, :].reshape(blocks, SPAN, state_width)
    d_blocks = delta.reshape(blocks, SPAN, heads_here)
    initial = jnp.zeros((heads_here, head_width, state_width), jnp.float32)
    final_state, outputs = lax.scan(
        partial(span_step, decay_rate, skip_scale),
        initial,
        (xs_blocks, b_blocks, c_blocks, d_blocks),
    )
    cumdev = jnp.cumsum(-delta * decay_rate[None, :], axis=0)
    totals = cumdev[-1]

    def combine(earlier, later):
        return (earlier[0] + later[0], jnp.exp(later[0])[:, None, None] * earlier[1] + later[1])

    scanned = prefix(
        (totals, final_state), "seq", combine, (jnp.zeros_like(totals), jnp.zeros_like(final_state))
    )
    incoming = scanned[1]
    cmat_wide = conv_out[:, 1, :].astype(jnp.float32)
    carried = jnp.exp(cumdev)[:, :, None] * jnp.einsum(
        "tn,hpn->thp", cmat_wide, incoming, precision=HIGH
    )
    mixed_heads = (outputs.reshape(tok_rows, heads_here, head_width) + carried).reshape(
        tok_rows, heads_here * head_width
    )
    gated = mixed_heads * jax.nn.silu(inner[:, 1, :].astype(jnp.float32))
    squares = lax.psum(jnp.sum(gated * gated, axis=1), "grp")
    row_scale = lax.rsqrt(squares / (lax.axis_size("grp") * gated.shape[1]) + EPS)
    scaled = (gated * out_gain).astype(jnp.bfloat16)
    summed = jnp.dot(
        lax.all_gather(scaled, "grp", axis=1, tiled=True),
        out_weight,
        preferred_element_type=jnp.float32,
    )
    return (summed * row_scale[:, None]).astype(jnp.bfloat16)


LANES = 128
TAIL = 16
AXES = ("seq", "grp")
F32 = jnp.float32
BF16 = jnp.bfloat16


class Places:
    def __init__(self):
        self.depth = lax.axis_size("seq") // 2
        self.width = lax.axis_size("grp") // 2
        seq, grp = lax.axis_index("seq"), lax.axis_index("grp")
        self.z, self.y, self.x, self.c = seq // 2, seq % 2, grp // 2, grp % 2

    def flat(self, z, y, x, c):
        return ((z * 2 + y) * self.width + x) * 2 + c

    def pairs(self, rule):
        out = []
        for z in range(self.depth):
            for y in range(2):
                for x in range(self.width):
                    for c in range(2):
                        target = rule(z, y, x, c)
                        if target is not None:
                            out.append((self.flat(z, y, x, c), self.flat(*target)))
        return out

    def send(self, value, rule):
        return lax.ppermute(value, AXES, self.pairs(rule))


def half_of(z):
    return z // 2


def spread_lanes(columns, first, second):
    rows = columns.shape[0]
    low = lax.broadcasted_iota(jnp.int32, (rows, LANES), 1) < LANES // 2
    a = jnp.broadcast_to(columns[:, first : first + 1], (rows, LANES))
    b = jnp.broadcast_to(columns[:, second : second + 1], (rows, LANES))
    return jnp.where(low, a, b)


def span_kernel(
    heads,
    pre_ref,
    tail_ref,
    raw_ref,
    scal_ref,
    cw_ref,
    cs_ref,
    skip_ref,
    y_ref,
    cmat_ref,
    grow_ref,
    state_ref,
    padded,
    state,
    gone,
):
    block = pl.program_id(0)
    rows = pre_ref.shape[0]
    wide = y_ref.shape[1]
    taps = 4
    n = cmat_ref.shape[1]

    @pl.when(block == 0)
    def _():
        padded[0:TAIL, :wide] = tail_ref[:, :wide].astype(F32)
        padded[0:TAIL, wide:] = tail_ref[:, 2 * wide :].astype(F32)
        state[...] = jnp.zeros_like(state)
        gone[...] = jnp.ones_like(gone)

    @pl.when(block > 0)
    def _():
        padded[0:TAIL, :] = padded[rows : rows + TAIL, :]

    padded[TAIL : TAIL + rows, :wide] = pre_ref[:, :wide].astype(F32)
    padded[TAIL : TAIL + rows, wide:] = pre_ref[:, 2 * wide :].astype(F32)

    def conv(start, stop, weight_ref, offset):
        total = jnp.zeros((rows, stop - start), F32)
        for j in range(taps):
            first = TAIL - taps + 1 + j
            total = total + weight_ref[j : j + 1, start - offset : stop - offset] * padded[
                first : first + rows, start:stop
            ]
        return (total * jax.nn.sigmoid(total)).astype(BF16)

    bmat = conv(wide, wide + n, cs_ref, wide)
    cmat = conv(wide + n, wide + 2 * n, cs_ref, wide)
    cmat_ref[...] = cmat

    raw = raw_ref[...] + scal_ref[:, 0:1]
    delta = jnp.maximum(raw, 0.0) + jnp.log1p(jnp.exp(-jnp.abs(raw)))
    cumul = -delta * scal_ref[:, 1:2]
    spot = lax.broadcasted_iota(jnp.int32, cumul.shape, 1)
    shift = 1
    while shift < rows:
        cumul = cumul + jnp.where(spot >= shift, pltpu.roll(cumul, shift, 1), 0.0)
        shift *= 2
    last = cumul[:, rows - 1 : rows]
    tail = jnp.exp(last - cumul) * delta
    stack = jnp.concatenate(
        [cumul, tail, jnp.zeros((LANES - 2 * cumul.shape[0], rows), F32)], axis=0
    )
    cols = stack.T
    cum_cols = cols[:, :16]
    grow_cols = jnp.exp(cum_cols)

    scores = lax.dot_general(cmat, bmat, (((1,), (1,)), ((), ())), preferred_element_type=F32)
    lower = lax.broadcasted_iota(jnp.int32, (rows, rows), 0) >= lax.broadcasted_iota(
        jnp.int32, (rows, rows), 1
    )
    scores = jnp.where(lower, scores, 0.0)
    lane = lax.broadcasted_iota(jnp.int32, (rows, LANES), 1)

    for pair in range(heads // 2):
        start = pair * LANES
        vals = conv(start, start + LANES, cw_ref, 0)
        wide_vals = vals.astype(F32)
        growth = spread_lanes(grow_cols, 2 * pair, 2 * pair + 1)
        carried = jnp.dot(
            cmat, state[:, start : start + LANES].astype(BF16), preferred_element_type=F32
        )
        total = growth * carried + skip_ref[0:1, start : start + LANES] * wide_vals
        for side in range(2):
            head = 2 * pair + side
            diff = cum_cols[:, head : head + 1] - cumul[head : head + 1, :]
            mixer = scores * jnp.exp(jnp.minimum(diff, 0.0)) * delta[head : head + 1, :]
            mine = (lane < LANES // 2) if side == 0 else (lane >= LANES // 2)
            part = jnp.where(mine, wide_vals, 0.0).astype(BF16)
            total = total + jnp.dot(mixer.astype(BF16), part, preferred_element_type=F32)
        y_ref[:, start : start + LANES] = total
        weighted = (wide_vals * spread_lanes(cols, 16 + 2 * pair, 17 + 2 * pair)).astype(BF16)
        update = lax.dot_general(
            bmat, weighted, (((0,), (0,)), ((), ())), preferred_element_type=F32
        )
        ratio = growth[rows - 1 : rows, :]
        state[:, start : start + LANES] = ratio * state[:, start : start + LANES] + update
        before = gone[0:1, start : start + LANES]
        grow_ref[:, start : start + LANES] = growth * before
        gone[:, start : start + LANES] = jnp.broadcast_to(before * ratio, (gone.shape[0], LANES))

    state_ref[0:n, :] = state[...]
    state_ref[n:, :] = gone[...]


def span_call(pre, raw, scalars, conv_w, conv_s, skip, heads, n):
    rows = raw.shape[1]
    wide = skip.shape[1]
    blocks = rows // SPAN
    full = lambda a: pl.BlockSpec(a.shape, lambda b: (0, 0))
    return pl.pallas_call(
        partial(span_kernel, heads),
        grid=(blocks,),
        in_specs=[
            pl.BlockSpec((SPAN, pre.shape[1]), lambda b: (b, 0)),
            pl.BlockSpec((TAIL, pre.shape[1]), lambda b: (rows // TAIL, 0)),
            pl.BlockSpec((raw.shape[0], SPAN), lambda b: (0, b)),
            full(scalars),
            full(conv_w),
            full(conv_s),
            full(skip),
        ],
        out_specs=[
            pl.BlockSpec((SPAN, wide), lambda b: (b, 0)),
            pl.BlockSpec((SPAN, n), lambda b: (b, 0)),
            pl.BlockSpec((SPAN, wide), lambda b: (b, 0)),
            pl.BlockSpec((n + 8, wide), lambda b: (0, 0)),
        ],
        out_shape=[
            jax.ShapeDtypeStruct((rows, wide), F32),
            jax.ShapeDtypeStruct((rows, n), BF16),
            jax.ShapeDtypeStruct((rows, wide), F32),
            jax.ShapeDtypeStruct((n + 8, wide), F32),
        ],
        scratch_shapes=[
            pltpu.VMEM((TAIL + SPAN, wide + 2 * n), F32),
            pltpu.VMEM((n, wide), F32),
            pltpu.VMEM((8, wide), F32),
        ],
        compiler_params=pltpu.CompilerParams(dimension_semantics=("arbitrary",)),
        cost_estimate=pl.CostEstimate(
            flops=4_000_000_000, bytes_accessed=6_000_000, transcendentals=0
        ),
    )(pre, pre, raw, scalars, conv_w, conv_s, skip)


def gate_kernel(y_ref, cmat_ref, grow_ref, gate_ref, state_ref, gain_ref, out_ref):
    rows = y_ref.shape[0]
    into = jnp.dot(cmat_ref[...], state_ref[...].astype(BF16), preferred_element_type=F32)
    gate = gate_ref[...].astype(F32)
    gated = (y_ref[...] + grow_ref[...] * into) * (gate * jax.nn.sigmoid(gate))
    out_ref[0:rows, :] = (gated * gain_ref[0:1, :]).astype(BF16)
    sums = jnp.sum(gated * gated, axis=1, keepdims=True)
    line = jnp.broadcast_to(sums, (rows, LANES)).T[0:8, :]
    out_ref[rows:, :] = jnp.zeros((out_ref.shape[0] - rows, out_ref.shape[1]), BF16)
    first = line.astype(BF16)
    rest = line - first.astype(F32)
    second = rest.astype(BF16)
    third = (rest - second.astype(F32)).astype(BF16)
    pick = lax.broadcasted_iota(jnp.int32, line.shape, 0)
    packed = jnp.where(
        pick == 0,
        first.astype(F32),
        jnp.where(pick == 1, second.astype(F32), jnp.where(pick == 2, third.astype(F32), 0.0)),
    )
    both = jnp.concatenate([packed, jnp.zeros_like(packed)], axis=0)
    out_ref[rows:, 0:rows] = both.astype(BF16)


def gate_call(y, cmat, grow, pre, state, gain):
    rows, wide = y.shape
    return pl.pallas_call(
        gate_kernel,
        grid=(1,),
        in_specs=[
            pl.BlockSpec((rows, wide), lambda b: (0, 0)),
            pl.BlockSpec(cmat.shape, lambda b: (0, 0)),
            pl.BlockSpec((rows, wide), lambda b: (0, 0)),
            pl.BlockSpec((rows, wide), lambda b: (0, 1)),
            pl.BlockSpec(state.shape, lambda b: (0, 0)),
            pl.BlockSpec(gain.shape, lambda b: (0, 0)),
        ],
        out_specs=pl.BlockSpec((rows + TAIL, wide), lambda b: (0, 0)),
        out_shape=jax.ShapeDtypeStruct((rows + TAIL, wide), BF16),
        cost_estimate=pl.CostEstimate(
            flops=500_000_000, bytes_accessed=6_000_000, transcendentals=0
        ),
    )(y, cmat, grow, pre, state, gain)


def body(
    tokens,
    norm_gain,
    inner_weight,
    state_weight,
    step_weight,
    step_bias,
    decay_rate,
    skip_scale,
    conv_inner,
    conv_state,
    out_gain,
    out_weight,
):
    here = Places()
    z, y, x, c = here.z, here.y, here.x, here.c
    rows, model = tokens.shape
    piece_rows = rows // 2
    heads_grp = step_bias.shape[0]
    heads_chip = heads_grp // here.depth
    heads = 2 * heads_chip
    own_ch = out_gain.shape[0] // here.depth
    wide = 2 * own_ch
    n = state_weight.shape[2]

    before = from_behind(tokens[rows - TAIL :], "seq", 1)

    turned = jnp.transpose(inner_weight, (1, 2, 0))
    other = here.send(turned, lambda z, y, x, c: (z, 1 - y, x, c))
    both = jnp.concatenate(
        [jnp.where(y == 0, turned, other), jnp.where(y == 0, other, turned)], axis=1
    )
    sibling = lambda z, y, x, c: (z, y, x, 1 - c)
    both_other = here.send(both, sibling)
    inner_w = jnp.concatenate(
        [jnp.where(c == 0, both, both_other), jnp.where(c == 0, both_other, both)], axis=1
    ).reshape(2 * wide, model)
    weights = jnp.concatenate(
        [inner_w, jnp.transpose(state_weight, (1, 2, 0)).reshape(2 * n, model)], axis=0
    )

    cut = lambda a, size: lax.dynamic_slice_in_dim(a, z * size, size, axis=0)
    small = jnp.concatenate(
        [
            lax.dynamic_slice_in_dim(conv_inner, z * own_ch, own_ch, axis=1)
            .astype(F32)
            .reshape(-1),
            cut(out_gain, own_ch),
            cut(step_bias, heads_chip),
            cut(decay_rate, heads_chip),
            cut(skip_scale, heads_chip),
        ]
    )
    small = jnp.pad(small, (0, model - small.shape[0]))[None]
    mine = jnp.concatenate([cut(step_weight.T, heads_chip).astype(F32), small], axis=0)
    theirs = here.send(mine, sibling)
    parts = [jnp.where(c == 0, mine, theirs), jnp.where(c == 0, theirs, mine)]
    step_t = jnp.concatenate(
        [p[:heads_chip] for p in parts] + [jnp.zeros((16 - heads, model), F32)], axis=0
    ).astype(BF16)
    taps = conv_inner.shape[0]
    lines = [p[heads_chip] for p in parts]
    conv_w = jnp.concatenate([v[: taps * own_ch].reshape(taps, own_ch) for v in lines], axis=1)
    at = taps * own_ch
    gain = jnp.concatenate([v[at : at + own_ch] for v in lines])[None]
    at += own_ch
    vectors = []
    for _ in range(3):
        vectors.append(jnp.concatenate([v[at : at + heads_chip] for v in lines]))
        at += heads_chip
    bias, rate, skip_heads = vectors
    skip = jnp.repeat(skip_heads, wide // heads)[None]
    scalars = jnp.pad(jnp.stack([bias, rate], axis=1), ((0, 16 - heads), (0, LANES - 2)))
    conv_s = conv_state.reshape(taps, 2 * n).astype(F32)

    ext = jnp.concatenate([tokens, before], axis=0).astype(F32)
    normed = (
        ext * lax.rsqrt(jnp.mean(ext * ext, axis=1, keepdims=True) + EPS) * norm_gain
    ).astype(BF16)
    tail = normed[rows:]
    half = jnp.concatenate(
        [lax.dynamic_slice_in_dim(normed, x * piece_rows, piece_rows, axis=0), tail], axis=0
    )

    def table_rule(table):
        def rule(z, y, x, c):
            if (z, c) not in table:
                return None
            z2, c2 = table[z, c]
            return (z2, y, x, c2)

        return rule

    tables = [
        {(0, 0): (1, 0), (1, 0): (2, 0), (1, 1): (0, 0), (2, 1): (3, 1), (2, 0): (1, 1), (3, 1): (2, 1)},
        {(1, 0): (2, 0), (2, 0): (3, 0), (2, 1): (1, 1), (1, 1): (0, 1)},
        {(2, 0): (3, 0), (1, 1): (0, 1)},
    ]
    shards = [normed]
    moving = half
    for table in tables:
        moving = here.send(moving, table_rule(table))
        reached = set(table.values())
        across = here.send(
            moving, lambda z, y, x, c: (z, y, 1 - x, c) if (z, c) in reached else None
        )
        low = jnp.where(x == 0, moving, across)
        high = jnp.where(x == 0, across, moving)
        shards.append(jnp.concatenate([low[:piece_rows], high], axis=0))

    away = jnp.where(c == 0, jnp.maximum(z - 1, 0), jnp.maximum(2 - z, 0))
    near_is_upper = jnp.where(c == 0, z >= 1, z >= 3)

    def one_shard(shard):
        pre = lax.dot_general(
            shard, weights, (((1,), (1,)), ((), ())), preferred_element_type=F32
        ).astype(BF16)
        raw = lax.dot_general(
            step_t, shard, (((1,), (1,)), ((), ())), preferred_element_type=F32
        )[:, :rows]
        return (pre, *span_call(pre, raw, scalars, conv_w, conv_s, skip, heads, n))

    near = one_shard(
        jnp.where(away == 0, shards[0], jnp.where(away == 1, shards[1], shards[2]))
    )
    far = one_shard(
        jnp.where(away == 0, shards[1], jnp.where(away == 1, shards[2], shards[3]))
    )

    first = jnp.where(near_is_upper, far[4], near[4])
    second = jnp.where(near_is_upper, near[4], far[4])
    swap_y = lambda z, y, x, c: (z, 1 - y, x, c)
    first_other, second_other = here.send(first, swap_y), here.send(second, swap_y)
    chain = [
        jnp.where(y == 0, first, first_other),
        jnp.where(y == 0, first_other, first),
        jnp.where(y == 0, second, second_other),
        jnp.where(y == 0, second_other, second),
    ]
    run = jnp.zeros((n, wide), F32)
    for link in chain:
        run = link[n : n + 1] * run + link[:n]
    run = here.send(run, lambda z, y, x, c: (z, y, x, 1) if c == 0 else None)
    into = []
    for link in chain:
        into.append(run)
        run = link[n : n + 1] * run + link[:n]
    into_first = jnp.where(y == 0, into[0], into[1])
    into_second = jnp.where(y == 0, into[2], into[3])

    near_out = gate_call(
        near[1], near[2], near[3], near[0], jnp.where(near_is_upper, into_second, into_first), gain
    )
    far_out = gate_call(
        far[1], far[2], far[3], far[0], jnp.where(near_is_upper, into_first, into_second), gain
    )
    lower = jnp.where(near_is_upper, far_out, near_out)
    upper = jnp.where(near_is_upper, near_out, far_out)

    depth = here.depth
    main = c == half_of(z)
    grouped = out_weight.reshape(here.width, 2, depth, own_ch, out_weight.shape[1])

    def rows_of(x_from, z_from):
        part = lax.dynamic_slice(
            grouped, (x_from, 0, z_from, 0, 0), (1, 2, 1, own_ch, out_weight.shape[1])
        )
        return part.reshape(wide, out_weight.shape[1])

    pieces, panels = [], []
    for k in range(depth):
        target = (z + k) % depth
        piece = jnp.where(target % 2 == 0, lower, upper)
        if k > 0:
            piece = here.send(
                piece,
                lambda z, y, x, c: ((z + k) % depth, y, x, c)
                if c == half_of((z + k) % depth)
                else None,
            )
        across = here.send(
            piece, lambda z, y, x, c: (z, y, 1 - x, c) if c == half_of(z) else None
        )
        for value, x_from in ((piece, x), (across, 1 - x)):
            copy = here.send(
                value, lambda z, y, x, c: (z, y, x, 1 - c) if c == half_of(z) else None
            )
            pieces.append(jnp.where(main, value, copy))
            panels.append(rows_of(x_from, (z - k) % depth))
    total = jnp.zeros((rows, out_weight.shape[1]), F32)
    squares = jnp.zeros((rows,), F32)
    for piece, panel in zip(pieces, panels):
        total = total + jnp.dot(piece[:rows], panel, preferred_element_type=F32)
        squares = squares + jnp.sum(piece[rows : rows + 3, :rows].astype(F32), axis=0)
    scale = lax.rsqrt(squares / (here.depth * here.width * wide) + EPS)
    return (total * scale[:, None]).astype(BF16)


def fits(mesh):
    return mesh.shape["seq"] == 8 and mesh.shape["grp"] == 4


def solution(mesh):
    return jax.shard_map(
        body if fits(mesh) else plain_body,
        mesh=mesh,
        in_specs=(
            P("seq", None),
            P(),
            P(None, None, ("grp", "seq")),
            P(),
            P(None, "grp"),
            P("grp"),
            P("grp"),
            P("grp"),
            P(None, "grp"),
            P(),
            P("grp"),
            P(None, "grp"),
        ),
        out_specs=P("seq", "grp"),
        check_vma=False,
    )
```
